32 devices in a mesh: seq: 8 (over y, x, core), sub: 4 (over z).
Axes of the slice: x: 2, y: 2, z: 4, core: 2. Of those that a mesh axis runs over, the one named last changes fastest.
Arguments:
- tokens: bfloat16 [2048, 4096], P('seq'), may hold values from -6 to 6
- w_split: bfloat16 [4096, 4096], P(None, 'sub'), may hold values from -0.09375 to 0.09375
- w_merge: bfloat16 [4096, 4096], P('sub'), may hold values from -0.09375 to 0.09375
- expert_in: bfloat16 [32, 1024, 2048], P(('seq', 'sub')), may hold values from -0.1875 to 0.1875
- expert_out: bfloat16 [32, 1024, 1024], P(('seq', 'sub')), may hold values from -0.1875 to 0.1875
- expert_ids: int32 [4, 2048, 2], P('sub', 'seq'), may hold values from 0 to 31, all different within a row; in each aligned block of 256 rows (0 to 255, 256 to 511, ..., all dimensions but the last counted through in order) at most 24 rows name the same one
- combine_q: int32 [4, 2048, 2], P('sub', 'seq'), may hold values from 4096 to 65536
- capacity: int32 [32], replicated, may hold values from 12 to 24
Outputs:
- mixed: bfloat16 [2048, 4096], P('seq', 'sub')
The draws below stay inside these ranges and needn't reach their ends.
Inputs may be any that keep to these rules, and one draw needn't show every extreme that they name: `expert_ids`: in each block of 256 positions of one sub-head, the ids of a position differ, no expert is named more than 24 times, a bound that some block reaches.
All inputs are finite; a program needn't handle non-finite values.
Results may differ from the reference program's by a relative error of at most 0.0076.
Values may be sent and summed in bfloat16 or wider, within the bound.
A program may use at most 128 MiB of HBM per device.

```python
import math
import jax
import jax.numpy as jnp
import numpy as np
from jax import lax

D = 4096
HEADS = 4
FFE = 1024
TOPK = 2
TOK_DEV = 256
SUBW = 1024
EXPERTS = 32
CAP = 24
TOKENS = 2048
N_SEQ = 8


def with_ends(entries, rng, smallest, high):
    longest = entries.shape.index(max(entries.shape))
    spots = []
    for shift in (0, 1):
        where = [jax.random.randint(jax.random.fold_in(rng, axis), (), 0, length) for axis, length in enumerate(entries.shape)]
        where[longest] = (where[longest] + shift) % entries.shape[longest]
        spots.append(tuple(where))
    return entries.at[spots[0]].set(smallest).at[spots[1]].set(high)


def shard_levels(key, extent, split, least, top_value):
    def one(axis_at, blocks):
        draws = jax.random.uniform(jax.random.fold_in(jax.random.fold_in(key, 6), axis_at), (blocks,), jnp.float32, least / len(split), top_value / len(split))
        return jnp.repeat(jnp.exp(draws), extent[axis_at] // blocks).reshape((-1,) + (1,) * (len(extent) - axis_at - 1))

    gain = one(*split[0])
    for cut in split[1:]:
        gain = gain * one(*cut)
    return gain


def deal_out(rng, own, number, rows, number_of, top, limit, lean):
    ranking = jax.random.permutation(rng, number_of)
    crowded, common = shares(number_of, rows * top, limit, lean, True), shares(number_of, rows * top, limit, lean, False)
    places = jnp.arange(number_of)

    def named(lengths, rotation):
        used = int((lengths > 0).sum())
        fixed = max(1, used // 4)
        moved = fixed + (places - fixed + rotation * (used - fixed)) % max(1, number_of - fixed)
        return jnp.zeros((number_of,), jnp.int32).at[ranking[jnp.where(places < fixed, places, moved)]].set(jnp.asarray(lengths, jnp.int32))

    lengths = jnp.where(number % 4 == 0, named(crowded, number // 4), named(common, number - number // 4 - 1))
    mixed = jax.random.permutation(jax.random.fold_in(own, 3), number_of)
    source_of, sink = mixed[0:number_of // 2 * 2:2], mixed[1:number_of // 2 * 2:2]
    slack = jnp.minimum(lengths[source_of] - 1, limit - lengths[sink]) // 2
    slack = jnp.where((source_of == ranking[0]) | (sink == ranking[0]) | (lengths[sink] == 0), 0, jnp.maximum(slack, 0))
    moved = jax.random.randint(jax.random.fold_in(own, 4), (number_of // 2,), 0, 1 << 20) % (slack + 1)
    lengths = lengths.at[source_of].add(-moved).at[sink].add(moved)
    members = jnp.searchsorted(jnp.cumsum(lengths), jnp.arange(rows * top), side="right").astype(jnp.int32)
    table = members.reshape(top, rows).T
    table = table[jax.random.permutation(jax.random.fold_in(own, 1), rows)]
    rotation = jax.random.randint(jax.random.fold_in(own, 2), (rows, 1), 0, top)
    return jnp.take_along_axis(table, (jnp.arange(top)[None, :] + rotation) % top, axis=1)


def shares(number_of, total, limit, slope, full):
    loads = [(1 << 20) // math.isqrt(rank ** slope) + 1 for rank in range(1, number_of + 1)]
    largest = limit if full else min(limit, max(-(-total // number_of), total * loads[0] // sum(loads)))
    least = 1 if total - largest >= number_of - 1 else 0
    counts, rest = [largest] + [least] * (number_of - 1), total - largest - least * (number_of - 1)
    while rest > 0:
        candidates = [i for i in range(1, number_of) if counts[i] < largest] or [i for i in range(1, number_of) if counts[i] < limit]
        mass, remaining = sum([loads[i] for i in candidates]), rest
        for i in candidates:
            addition = min(limit - counts[i], max(1, remaining * loads[i] // mass), rest)
            counts[i] = counts[i] + addition
            rest = rest - addition
    return np.array(counts)


def centred(key, shape, scale, bound, split=(), kind=jnp.bfloat16):
    array = scale * jax.random.normal(key, shape, jnp.float32)
    if split:
        array = array * shard_levels(key, shape, split, -0.22, 0.18)
    return jnp.clip(array, -bound, bound).astype(kind)


def setup_inputs(seed: int = 0) -> dict:
    key_of = jax.random.split(jax.random.key(seed), 9)
    tokens = centred(key_of[0], (TOKENS, D), 1.0, 6.0, ((0, 8),))
    w_split = centred(key_of[1], (D, D), D ** -0.5, 0.09375, ((1, 4),))
    w_merge = centred(key_of[2], (D, D), D ** -0.5, 0.09375, ((0, 4),))
    expert_in = centred(key_of[3], (EXPERTS, SUBW, 2 * FFE), SUBW ** -0.5, 0.1875, ((0, 32),))
    expert_out = centred(key_of[4], (EXPERTS, FFE, SUBW), FFE ** -0.5, 0.1875, ((0, 32),))
    expert_ids_keys = jax.random.split(jax.random.fold_in(key_of[5], 1), HEADS * TOKENS // TOK_DEV)
    expert_ids_turns = jax.random.permutation(jax.random.fold_in(key_of[5], 3), HEADS * TOKENS // TOK_DEV)
    expert_ids = jax.vmap(lambda own, number: deal_out(jax.random.fold_in(key_of[5], 2), own, number, TOK_DEV, EXPERTS, TOPK, CAP, 2))(expert_ids_keys, expert_ids_turns).reshape((HEADS, TOKENS, TOPK))
    combine_q = with_ends(jax.random.randint(key_of[6], (HEADS, TOKENS, TOPK), 4096, 65537), jax.random.fold_in(key_of[6], 1), 4096, 65536).astype(jnp.int32)
    capacity = with_ends(jax.random.randint(key_of[7], (EXPERTS,), CAP // 2, CAP + 1), jax.random.fold_in(key_of[7], 1), CAP // 2, CAP).astype(jnp.int32)
    return {"tokens": tokens, "w_split": w_split, "w_merge": w_merge, "expert_in": expert_in, "expert_out": expert_out, "expert_ids": expert_ids, "combine_q": combine_q, "capacity": capacity}


def expert_ffn(inputs, w_in, w_out):
    gate_up = jnp.dot(inputs, w_in, preferred_element_type=jnp.float32)
    ffe_width = w_out.shape[0]
    hidden = (jax.nn.silu(gate_up[:, :ffe_width]) * gate_up[:, ffe_width:]).astype(jnp.bfloat16)
    return jnp.dot(hidden, w_out, preferred_element_type=jnp.float32).astype(jnp.bfloat16)


def reference(tokens, w_split, w_merge, expert_in, expert_out, expert_ids, combine_q, capacity):
    sub_tokens = jnp.dot(tokens, w_split, preferred_element_type=jnp.float32).astype(jnp.bfloat16)
    table = sub_tokens.reshape(TOKENS, HEADS, SUBW).transpose(1, 0, 2).reshape(HEADS * TOKENS, SUBW)
    block_count = HEADS * N_SEQ
    expert_of = expert_ids.reshape(block_count, TOPK * TOK_DEV)
    onehot = (expert_of[:, :, None] == jnp.arange(EXPERTS, dtype=jnp.int32)[None, None, :]).astype(jnp.int32)
    order_rank = jnp.sum((jnp.cumsum(onehot, axis=1) - onehot) * onehot, axis=2)
    cap_limit = jnp.sum(onehot * capacity[None, None, :], axis=2)
    is_kept = order_rank < cap_limit
    block_id = jnp.arange(block_count, dtype=jnp.int32)[:, None]
    slot_index = (expert_of * block_count + block_id) * CAP + order_rank
    total_slots = EXPERTS * block_count * CAP
    slot_index = jnp.where(is_kept, slot_index, total_slots)
    entry_pos = jnp.arange(TOPK * TOK_DEV, dtype=jnp.int32)[None, :]
    row_index = block_id * TOK_DEV + entry_pos // TOPK
    weights = combine_q.reshape(block_count, TOPK * TOK_DEV).astype(jnp.float32) / 65536.0
    slot_row = jnp.full((total_slots,), -1, jnp.int32).at[slot_index.reshape(-1)].set(
        jnp.broadcast_to(row_index, slot_index.shape).reshape(-1), mode="drop")
    slot_weight = jnp.zeros((total_slots,), jnp.float32).at[slot_index.reshape(-1)].set(
        weights.reshape(-1), mode="drop")
    slot_row = slot_row.reshape(EXPERTS, block_count * CAP)
    slot_weight = slot_weight.reshape(EXPERTS, block_count * CAP)

    def one_expert(running, inputs_e):
        rows_here, weights_here, w_in, w_out = inputs_e
        is_valid = rows_here >= 0
        safe_row = jnp.maximum(rows_here, 0)
        picked = jnp.where(is_valid[:, None], table[safe_row], jnp.zeros((), jnp.bfloat16))
        answer = expert_ffn(picked, w_in, w_out)
        weighted = jnp.where(is_valid[:, None], weights_here[:, None] * answer.astype(jnp.float32), jnp.zeros((), jnp.float32))
        return running.at[safe_row].add(weighted), None

    start = jnp.zeros((HEADS * TOKENS, SUBW), jnp.float32)
    running, _ = lax.scan(one_expert, start, (slot_row, slot_weight, expert_in, expert_out))
    head_out = running.astype(jnp.bfloat16).reshape(HEADS, TOKENS, SUBW).transpose(1, 0, 2).reshape(TOKENS, D)
    return jnp.dot(head_out, w_merge, preferred_element_type=jnp.float32).astype(jnp.bfloat16)
```

```python
import functools

import jax
import jax.numpy as jnp
from jax import lax
from jax.experimental import pallas as pl
from jax.experimental.pallas import tpu as pltpu
from jax.sharding import PartitionSpec as P

MESH = pl.DeviceIdType.MESH
GROUPS = 4
TILE = 256
CHUNKS = 2
VMEM_LIMIT = 48 * 1024 * 1024


def experts_kernel(n_seq, n_sub, packed, w_in, w_out, returned, received, answers, hidden,
                   send_sem, recv_sem, back_sem, ret_sem):
    n = n_seq * n_sub
    me = lax.axis_index("seq") * n_sub + lax.axis_index("sub")
    block = packed.shape[0] // n
    half = packed.shape[1]
    slots = block // 2
    per = n // GROUPS
    ffe = w_out.shape[0]

    def rows(i):
        return pl.ds(pl.multiple_of(i * block, 16), block)

    def device(i):
        return (i // n_sub, lax.rem(i, n_sub))

    def outgoing(i):
        target = lax.rem(me + i, n)
        return pltpu.make_async_remote_copy(
            src_ref=packed.at[rows(target)], dst_ref=received.at[rows(i)],
            send_sem=send_sem.at[i], recv_sem=recv_sem.at[i],
            device_id=device(target), device_id_type=MESH)

    def homeward(i):
        source = lax.rem(me + n - i, n)
        return pltpu.make_async_remote_copy(
            src_ref=answers.at[rows(i)], dst_ref=returned.at[rows(me)],
            send_sem=back_sem.at[i], recv_sem=ret_sem.at[i],
            device_id=device(source), device_id_type=MESH)

    @pl.loop(1, n)
    def _(i):
        outgoing(i).start()

    received[0:block, :] = packed[rows(me), :]

    @pl.loop(0, GROUPS)
    def _(g):
        first = g * per
        low = jnp.where(g == 0, 1, first)

        @pl.loop(low, first + per)
        def _(i):
            outgoing(i).wait_recv()

        span = pl.ds(pl.multiple_of(first * block, 16), per * block)
        x = received[span, :].astype(jnp.float32).reshape(per, block, half)
        x = jnp.concatenate(
            [x[:, :slots].reshape(per * slots, half), x[:, slots:].reshape(per * slots, half)],
            axis=1).astype(jnp.bfloat16)

        @pl.loop(0, ffe // TILE)
        def _(c):
            gate_at = pl.ds(pl.multiple_of(c * TILE, TILE), TILE)
            up_at = pl.ds(pl.multiple_of(ffe + c * TILE, TILE), TILE)
            gate = jnp.dot(x, w_in[:, gate_at], preferred_element_type=jnp.float32)
            up = jnp.dot(x, w_in[:, up_at], preferred_element_type=jnp.float32)
            hidden[:, gate_at] = (gate / (1.0 + jnp.exp(-gate)) * up).astype(jnp.bfloat16)

        act = hidden[...]
        parts = []
        for h in range(2):
            y = jnp.dot(act, w_out[:, h * half:(h + 1) * half],
                        preferred_element_type=jnp.float32)
            parts.append(y.reshape(per, slots, half))
        y = jnp.concatenate(parts, axis=1).reshape(per * block, half)
        answers[span, :] = y.astype(jnp.bfloat16)

        @pl.loop(low, first + per)
        def _(i):
            homeward(i).start()

    returned[rows(me), :] = answers[0:block, :]

    @pl.loop(1, n)
    def _(i):
        outgoing(i).wait_send()
        homeward(i).wait_send()
        homeward(i).wait_recv()


def exchange_experts(n_seq, n_sub, packed, w_in, w_out):
    n = n_seq * n_sub
    width = w_out.shape[0]
    vmem = pl.BlockSpec(memory_space=pltpu.VMEM)
    rows = packed.shape[0] // 2 // GROUPS
    return pl.pallas_call(
        functools.partial(experts_kernel, n_seq, n_sub),
        out_shape=jax.ShapeDtypeStruct(packed.shape, jnp.bfloat16),
        in_specs=[vmem] * 3,
        out_specs=vmem,
        scratch_shapes=[
            pltpu.VMEM(packed.shape, jnp.bfloat16),
            pltpu.VMEM(packed.shape, jnp.bfloat16),
            pltpu.VMEM((rows, width), jnp.bfloat16),
        ] + [pltpu.SemaphoreType.DMA((n,))] * 4,
        compiler_params=pltpu.CompilerParams(has_side_effects=True, vmem_limit_bytes=VMEM_LIMIT),
        name="experts",
    )(packed, w_in, w_out)


def merge_kernel(n, head, w_hbm, out, w, total, sending, landed, w_sem, send_sem, recv_sem):
    z = lax.axis_index("sub")
    rows, width = out.shape
    piece = rows // CHUNKS

    def target(j):
        near_low = jnp.where(j < n - 1 - z, n - 1 - j, j - (n - 1 - z))
        near_high = jnp.where(j < z, j, n - 1 - (j - z))
        return jnp.where(z < n // 2, near_low, near_high)

    def fetch(j):
        t = target(j)
        return pltpu.make_async_copy(
            w_hbm.at[:, pl.ds(pl.multiple_of(t * width, width), width)], w.at[t], w_sem.at[j])

    for j in range(n):
        fetch(j).start()

    barrier = pltpu.get_barrier_semaphore()

    @pl.when(z > 0)
    def _():
        pl.semaphore_signal(barrier, inc=1, device_id={"sub": z - 1}, device_id_type=MESH)

    @pl.when(z < n - 1)
    def _():
        pl.semaphore_signal(barrier, inc=1, device_id={"sub": z + 1}, device_id_type=MESH)

    pl.semaphore_wait(barrier, jnp.where(z > 0, 1, 0) + jnp.where(z < n - 1, 1, 0))

    def hop(way, t, c):
        part = pl.ds(c * piece, piece)
        return pltpu.make_async_remote_copy(
            src_ref=sending.at[t, part], dst_ref=landed.at[way, t, part],
            send_sem=send_sem.at[t, c], recv_sem=recv_sem.at[way, t, c],
            device_id={"sub": z + (1 if way == 0 else -1)}, device_id_type=MESH)

    for j in range(n):
        t = target(j)
        fetch(j).wait()

        @pl.loop(0, width // TILE)
        def _(k):
            cols = pl.ds(pl.multiple_of(k * TILE, TILE), TILE)
            total[t, :, cols] = jnp.dot(head[...], w[t, :, cols],
                                        preferred_element_type=jnp.float32)

        for way, source in ((0, 0), (1, n - 1)):
            @pl.when((z == source) & (t != z))
            def _():
                for c in range(CHUNKS):
                    part = pl.ds(c * piece, piece)
                    sending[t, part, :] = total[t, part, :].astype(jnp.bfloat16)
                    hop(way, t, c).start()

    for k in range(n - 2):
        for c in range(CHUNKS):
            part = pl.ds(c * piece, piece)
            for way, t in ((0, n - 1 - k), (1, k)):
                inside = (z > 0) & (z < t) if way == 0 else (z < n - 1) & (z > t)

                @pl.when(inside)
                def _():
                    hop(way, t, c).wait_recv()
                    sending[t, part, :] = (
                        total[t, part, :] + landed[way, t, part, :].astype(jnp.float32)
                    ).astype(jnp.bfloat16)
                    hop(way, t, c).start()

    for way, has in ((0, z > 0), (1, z < n - 1)):
        @pl.when(has)
        def _():
            for c in range(CHUNKS):
                part = pl.ds(c * piece, piece)
                hop(way, z, c).wait_recv()
                total[z, part, :] += landed[way, z, part, :].astype(jnp.float32)

    out[...] = total[z].astype(out.dtype)
    for t in range(n):
        @pl.when(z < t)
        def _():
            for c in range(CHUNKS):
                hop(0, t, c).wait_send()

        @pl.when(z > t)
        def _():
            for c in range(CHUNKS):
                hop(1, t, c).wait_send()


def merge_scatter(n, head, w_merge):
    rows, width = head.shape[0], w_merge.shape[1] // n
    depth = w_merge.shape[0]
    vmem = pl.BlockSpec(memory_space=pltpu.VMEM)
    return pl.pallas_call(
        functools.partial(merge_kernel, n),
        out_shape=jax.ShapeDtypeStruct((rows, width), jnp.bfloat16),
        in_specs=[vmem, pl.BlockSpec(memory_space=pl.ANY)],
        out_specs=vmem,
        scratch_shapes=[
            pltpu.VMEM((n, depth, width), jnp.bfloat16),
            pltpu.VMEM((n, rows, width), jnp.float32),
            pltpu.VMEM((n, rows, width), jnp.bfloat16),
            pltpu.VMEM((2, n, rows, width), jnp.bfloat16),
            pltpu.SemaphoreType.DMA((n,)),
            pltpu.SemaphoreType.DMA((n, CHUNKS)),
            pltpu.SemaphoreType.DMA((2, n, CHUNKS)),
        ],
        compiler_params=pltpu.CompilerParams(
            collective_id=1, has_side_effects=True, vmem_limit_bytes=VMEM_LIMIT),
        name="merge",
    )(head, w_merge)


def body(n_seq, n_sub, tokens, w_split, w_merge, expert_in, expert_out, expert_ids, combine_q,
         capacity):
    sub_tok = jnp.dot(tokens, w_split, preferred_element_type=jnp.float32).astype(jnp.bfloat16)
    tok_rows = tokens.shape[0]
    experts = capacity.shape[0]
    slot_count = -(-(3 * tok_rows // experts) // 8) * 8
    expert_of = expert_ids[0].reshape(-1)
    onehot = (expert_of[:, None] == jnp.arange(experts, dtype=jnp.int32)[None, :]).astype(jnp.int32)
    order_rank = jnp.sum((jnp.cumsum(onehot, axis=0) - onehot) * onehot, axis=1)
    cap_limit = jnp.sum(onehot * capacity[None, :], axis=1)
    is_kept = order_rank < cap_limit
    place = jnp.where(is_kept, expert_of * (2 * slot_count) + order_rank, -(4 * slot_count))
    place = place.reshape(tok_rows, -1)
    half = sub_tok.shape[1] // 2
    target = jnp.arange(experts * 2 * slot_count, dtype=jnp.int32)
    both = jnp.concatenate([place, place + slot_count], axis=0)
    chosen = (
        (target[:, None] == both[None, :, 0]) | (target[:, None] == both[None, :, 1])
    ).astype(jnp.bfloat16)
    stacked = jnp.concatenate([sub_tok[:, :half], sub_tok[:, half:]], axis=0)
    packed = jnp.dot(chosen, stacked, preferred_element_type=jnp.float32).astype(jnp.bfloat16)
    returned = exchange_experts(n_seq, n_sub, packed, expert_in[0], expert_out[0])
    weight = combine_q[0].astype(jnp.float32) / 65536.0
    twice = jnp.concatenate([weight, weight], axis=0)
    spread = (
        jnp.where(both[:, 0:1] == target[None, :], twice[:, 0:1], 0.0)
        + jnp.where(both[:, 1:2] == target[None, :], twice[:, 1:2], 0.0)
    )
    high = spread.astype(jnp.bfloat16)
    low = (spread - high.astype(jnp.float32)).astype(jnp.bfloat16)
    summed = (jnp.dot(high, returned, preferred_element_type=jnp.float32)
              + jnp.dot(low, returned, preferred_element_type=jnp.float32))
    head_out = jnp.concatenate([summed[:tok_rows], summed[tok_rows:]], axis=1).astype(jnp.bfloat16)
    return merge_scatter(n_sub, head_out, w_merge)


def solution(mesh):
    in_specs = (
        P("seq", None),
        P(None, "sub"),
        P("sub", None),
        P(("seq", "sub"), None, None),
        P(("seq", "sub"), None, None),
        P("sub", "seq", None),
        P("sub", "seq", None),
        P(),
    )
    out_specs = P("seq", "sub")
    call = functools.partial(body, mesh.shape["seq"], mesh.shape["sub"])
    return jax.shard_map(call, mesh=mesh, in_specs=in_specs, out_specs=out_specs, check_vma=False)
```

```python
import functools

import jax
import jax.numpy as jnp
from jax import lax
from jax.experimental import pallas as pl
from jax.experimental.pallas import tpu as pltpu
from jax.sharding import PartitionSpec as P

MESH = pl.DeviceIdType.MESH
GROUPS = 4
TILE = 256
CHUNKS = 2
EXPERTS_VMEM = 28 * 1024 * 1024
MERGE_VMEM = 28 * 1024 * 1024


def experts_kernel(n_seq, n_sub, slots, sub_tok, ids, quanta, capacity, w_in_hbm, w_out_hbm, head,
                   packed, received, answers, returned, hidden, w_in, w_out, w_sem,
                   send_sem, recv_sem, back_sem, ret_sem):
    n = n_seq * n_sub
    me = lax.axis_index("seq") * n_sub + lax.axis_index("sub")
    tok_rows, width = sub_tok.shape
    half = width // 2
    block = 2 * slots
    per = n // GROUPS
    ffe = w_out.shape[0]

    fetch_in = pltpu.make_async_copy(w_in_hbm, w_in, w_sem.at[0])
    fetch_out = pltpu.make_async_copy(w_out_hbm, w_out, w_sem.at[1])

    def rows(i):
        return pl.ds(pl.multiple_of(i * block, 16), block)

    def span(g):
        return pl.ds(pl.multiple_of(g * per * block, 16), per * block)

    def device(i):
        return (i // n_sub, lax.rem(i, n_sub))

    def outgoing(i):
        return pltpu.make_async_remote_copy(
            src_ref=packed.at[rows(i)], dst_ref=received.at[rows(i)],
            send_sem=send_sem.at[i], recv_sem=recv_sem.at[i],
            device_id=device(lax.rem(me + i, n)), device_id_type=MESH)

    def homeward(i):
        return pltpu.make_async_remote_copy(
            src_ref=answers.at[rows(i)], dst_ref=returned.at[rows(i)],
            send_sem=back_sem.at[i], recv_sem=ret_sem.at[i],
            device_id=device(lax.rem(me + n - i, n)), device_id_type=MESH)

    def fold(y):
        y = y.reshape(per, slots, width)
        y = jnp.concatenate([y[:, :, :half], y[:, :, half:]], axis=1)
        return y.reshape(per * block, half).astype(jnp.bfloat16)

    def unfold(x):
        x = x.astype(jnp.float32).reshape(per, block, half)
        return jnp.concatenate(
            [x[:, :slots].reshape(per * slots, half), x[:, slots:].reshape(per * slots, half)],
            axis=1).astype(jnp.bfloat16)

    places = lax.broadcasted_iota(jnp.int32, (n, tok_rows), 0)
    named = [(places == ids[k:k + 1, :]).astype(jnp.float32) for k in range(2)]
    before = (lax.broadcasted_iota(jnp.int32, (tok_rows, tok_rows), 0)
              < lax.broadcasted_iota(jnp.int32, (tok_rows, tok_rows), 1))
    earlier = jnp.dot((named[0] + named[1]).astype(jnp.bfloat16),
                      before.astype(jnp.float32).astype(jnp.bfloat16),
                      preferred_element_type=jnp.float32)
    limit = capacity[...].astype(jnp.float32)
    slot, weight = [], []
    for k in range(2):
        rank = jnp.sum(named[k] * earlier, axis=0, keepdims=True)
        most = jnp.sum(named[k] * limit, axis=0, keepdims=True)
        away = ids[k:k + 1, :] - me
        away = jnp.where(away < 0, away + n, away)
        slot.append(jnp.where(rank < most, away * slots + rank.astype(jnp.int32), -1))
        weight.append(quanta[k:k + 1, :].astype(jnp.float32) / 65536.0)

    def spread(g, values):
        at = lax.broadcasted_iota(jnp.int32, (per * slots, tok_rows), 0) + g * (per * slots)
        return (jnp.where(at == slot[0], values[0], 0.0)
                + jnp.where(at == slot[1], values[1], 0.0))

    for g in range(GROUPS):
        chosen = spread(g, (1.0, 1.0)).astype(jnp.bfloat16)
        packed[span(g), :] = fold(jnp.dot(chosen, sub_tok[...],
                                          preferred_element_type=jnp.float32))

        @pl.loop(max(1, g * per), (g + 1) * per)
        def _(i):
            outgoing(i).start()

        if g == 0:
            fetch_in.start()
            fetch_out.start()

    received[0:block, :] = packed[0:block, :]
    fetch_in.wait()
    fetch_out.wait()

    @pl.loop(0, GROUPS)
    def _(g):
        first = g * per
        low = jnp.where(g == 0, 1, first)

        @pl.loop(low, first + per)
        def _(i):
            outgoing(i).wait_recv()

        x = unfold(received[span(g), :])

        @pl.loop(0, ffe // TILE)
        def _(c):
            gate_at = pl.ds(pl.multiple_of(c * TILE, TILE), TILE)
            up_at = pl.ds(pl.multiple_of(ffe + c * TILE, TILE), TILE)
            gate = jnp.dot(x, w_in[:, gate_at], preferred_element_type=jnp.float32)
            up = jnp.dot(x, w_in[:, up_at], preferred_element_type=jnp.float32)
            hidden[:, gate_at] = (gate / (1.0 + jnp.exp(-gate)) * up).astype(jnp.bfloat16)

        act = hidden[...]
        parts = []
        for h in range(2):
            y = jnp.dot(act, w_out[:, h * half:(h + 1) * half],
                        preferred_element_type=jnp.float32)
            parts.append(y.reshape(per, slots, half))
        y = jnp.concatenate(parts, axis=1).reshape(per * block, half)
        answers[span(g), :] = y.astype(jnp.bfloat16)

        @pl.loop(low, first + per)
        def _(i):
            homeward(i).start()

    returned[0:block, :] = answers[0:block, :]
    summed = jnp.zeros((tok_rows, width), jnp.float32)
    for g in range(GROUPS):
        @pl.loop(max(1, g * per), (g + 1) * per)
        def _(i):
            homeward(i).wait_recv()

        full = spread(g, weight)
        high = full.astype(jnp.bfloat16)
        low = (full - high.astype(jnp.float32)).astype(jnp.bfloat16)
        y = unfold(returned[span(g), :])
        for part in (high, low):
            summed = summed + lax.dot_general(part, y, (((0,), (0,)), ((), ())),
                                              preferred_element_type=jnp.float32)
    head[...] = summed.astype(jnp.bfloat16)

    @pl.loop(1, n)
    def _(i):
        outgoing(i).wait_send()
        homeward(i).wait_send()


def exchange_experts(n_seq, n_sub, slots, sub_tok, ids, quanta, capacity, w_in, w_out):
    n = n_seq * n_sub
    width = w_out.shape[1]
    vmem = pl.BlockSpec(memory_space=pltpu.VMEM)
    hbm = pl.BlockSpec(memory_space=pltpu.HBM)
    rows = n * slots // GROUPS
    crossing = pltpu.VMEM((n * 2 * slots, width // 2), jnp.bfloat16)
    return pl.pallas_call(
        functools.partial(experts_kernel, n_seq, n_sub, slots),
        out_shape=jax.ShapeDtypeStruct(sub_tok.shape, jnp.bfloat16),
        in_specs=[vmem] * 4 + [hbm] * 2,
        out_specs=vmem,
        scratch_shapes=[crossing] * 4 + [
            pltpu.VMEM((rows, w_out.shape[0]), jnp.bfloat16),
            pltpu.VMEM(w_in.shape, jnp.bfloat16),
            pltpu.VMEM(w_out.shape, jnp.bfloat16),
            pltpu.SemaphoreType.DMA((2,)),
        ] + [pltpu.SemaphoreType.DMA((n,))] * 4,
        compiler_params=pltpu.CompilerParams(
            has_side_effects=True, vmem_limit_bytes=EXPERTS_VMEM),
        name="experts",
    )(sub_tok, ids, quanta, capacity, w_in, w_out)


def merge_kernel(n, head, w, out, total, sending, landed, send_sem, recv_sem):
    z = lax.axis_index("sub")
    rows, width = out.shape
    piece = rows // CHUNKS

    def target(j):
        near_low = jnp.where(j < n - 1 - z, n - 1 - j, j - (n - 1 - z))
        near_high = jnp.where(j < z, j, n - 1 - (j - z))
        return jnp.where(z < n // 2, near_low, near_high)

    barrier = pltpu.get_barrier_semaphore()

    @pl.when(z > 0)
    def _():
        pl.semaphore_signal(barrier, inc=1, device_id={"sub": z - 1}, device_id_type=MESH)

    @pl.when(z < n - 1)
    def _():
        pl.semaphore_signal(barrier, inc=1, device_id={"sub": z + 1}, device_id_type=MESH)

    pl.semaphore_wait(barrier, jnp.where(z > 0, 1, 0) + jnp.where(z < n - 1, 1, 0))

    def hop(way, t, c):
        part = pl.ds(c * piece, piece)
        return pltpu.make_async_remote_copy(
            src_ref=sending.at[t, part], dst_ref=landed.at[way, t, part],
            send_sem=send_sem.at[t, c], recv_sem=recv_sem.at[way, t, c],
            device_id={"sub": z + (1 if way == 0 else -1)}, device_id_type=MESH)

    for j in range(n):
        t = target(j)

        @pl.loop(0, width // TILE)
        def _(k):
            cols = pl.ds(pl.multiple_of(k * TILE, TILE), TILE)
            from_cols = pl.ds(pl.multiple_of(t * width + k * TILE, TILE), TILE)
            total[t, :, cols] = jnp.dot(head[...], w[:, from_cols],
                                        preferred_element_type=jnp.float32)

        for way, source in ((0, 0), (1, n - 1)):
            @pl.when((z == source) & (t != z))
            def _():
                for c in range(CHUNKS):
                    part = pl.ds(c * piece, piece)
                    sending[t, part, :] = total[t, part, :].astype(jnp.bfloat16)
                    hop(way, t, c).start()

    for k in range(n - 2):
        for c in range(CHUNKS):
            part = pl.ds(c * piece, piece)
            for way, t in ((0, n - 1 - k), (1, k)):
                inside = (z > 0) & (z < t) if way == 0 else (z < n - 1) & (z > t)

                @pl.when(inside)
                def _():
                    hop(way, t, c).wait_recv()
                    sending[t, part, :] = (
                        total[t, part, :] + landed[way, t, part, :].astype(jnp.float32)
                    ).astype(jnp.bfloat16)
                    hop(way, t, c).start()

    for way, has in ((0, z > 0), (1, z < n - 1)):
        @pl.when(has)
        def _():
            for c in range(CHUNKS):
                part = pl.ds(c * piece, piece)
                hop(way, z, c).wait_recv()
                total[z, part, :] += landed[way, z, part, :].astype(jnp.float32)

    out[...] = total[z].astype(out.dtype)
    for t in range(n):
        @pl.when(z < t)
        def _():
            for c in range(CHUNKS):
                hop(0, t, c).wait_send()

        @pl.when(z > t)
        def _():
            for c in range(CHUNKS):
                hop(1, t, c).wait_send()


def merge_scatter(n, head, w_merge):
    rows, width = head.shape[0], w_merge.shape[1] // n
    vmem = pl.BlockSpec(memory_space=pltpu.VMEM)
    return pl.pallas_call(
        functools.partial(merge_kernel, n),
        out_shape=jax.ShapeDtypeStruct((rows, width), jnp.bfloat16),
        in_specs=[vmem, vmem],
        out_specs=vmem,
        scratch_shapes=[
            pltpu.VMEM((n, rows, width), jnp.float32),
            pltpu.VMEM((n, rows, width), jnp.bfloat16),
            pltpu.VMEM((2, n, rows, width), jnp.bfloat16),
            pltpu.SemaphoreType.DMA((n, CHUNKS)),
            pltpu.SemaphoreType.DMA((2, n, CHUNKS)),
        ],
        compiler_params=pltpu.CompilerParams(
            collective_id=1, has_side_effects=True, vmem_limit_bytes=MERGE_VMEM),
        name="merge",
    )(head, w_merge)


def body(n_seq, n_sub, tokens, w_split, w_merge, expert_in, expert_out, expert_ids, combine_q,
         capacity):
    sub_tok = jnp.dot(tokens, w_split, preferred_element_type=jnp.float32).astype(jnp.bfloat16)
    sub_tok, w_merge = lax.optimization_barrier((sub_tok, w_merge))
    tok_rows = tokens.shape[0]
    experts = capacity.shape[0]
    slot_count = -(-(3 * tok_rows // experts) // 8) * 8
    head_out = exchange_experts(
        n_seq, n_sub, slot_count, sub_tok, expert_ids[0].T, combine_q[0].T, capacity[:, None],
        expert_in[0], expert_out[0])
    return merge_scatter(n_sub, head_out, w_merge)


def solution(mesh):
    in_specs = (
        P("seq", None),
        P(None, "sub"),
        P("sub", None),
        P(("seq", "sub"), None, None),
        P(("seq", "sub"), None, None),
        P("sub", "seq", None),
        P("sub", "seq", None),
        P(),
    )
    out_specs = P("seq", "sub")
    call = functools.partial(body, mesh.shape["seq"], mesh.shape["sub"])
    return jax.shard_map(call, mesh=mesh, in_specs=in_specs, out_specs=out_specs, check_vma=False)
```

```python
import functools

import jax
import jax.numpy as jnp
from jax import lax
from jax.experimental import pallas as pl
from jax.experimental.pallas import tpu as pltpu
from jax.sharding import PartitionSpec as P

MESH = pl.DeviceIdType.MESH
GROUPS = 4
TILE = 256
CHUNKS = 2
EXPERTS_VMEM = 28 * 1024 * 1024
MERGE_VMEM = 28 * 1024 * 1024


def experts_kernel(n_seq, n_sub, slots, sub_tok, ids, quanta, capacity, w_in_hbm, w_out_hbm, head,
                   packed, received, answers, returned, hidden, w_in, w_out, w_sem,
                   send_sem, recv_sem, back_sem, ret_sem):
    n = n_seq * n_sub
    me = lax.axis_index("seq") * n_sub + lax.axis_index("sub")
    tok_rows, width = sub_tok.shape
    half = width // 2
    block = 2 * slots
    per = n // GROUPS
    ffe = w_out.shape[0]

    fetch_in = pltpu.make_async_copy(w_in_hbm, w_in, w_sem.at[0])
    fetch_out = pltpu.make_async_copy(w_out_hbm, w_out, w_sem.at[1])

    def rows(i):
        return pl.ds(pl.multiple_of(i * block, 16), block)

    def span(g):
        return pl.ds(pl.multiple_of(g * per * block, 16), per * block)

    def device(i):
        return (i // n_sub, lax.rem(i, n_sub))

    def outgoing(i):
        return pltpu.make_async_remote_copy(
            src_ref=packed.at[rows(i)], dst_ref=received.at[rows(i)],
            send_sem=send_sem.at[i], recv_sem=recv_sem.at[i],
            device_id=device(lax.rem(me + i, n)), device_id_type=MESH)

    def homeward(i):
        return pltpu.make_async_remote_copy(
            src_ref=answers.at[rows(i)], dst_ref=returned.at[rows(i)],
            send_sem=back_sem.at[i], recv_sem=ret_sem.at[i],
            device_id=device(lax.rem(me + n - i, n)), device_id_type=MESH)

    def fold(y):
        y = y.reshape(per, slots, width)
        y = jnp.concatenate([y[:, :, :half], y[:, :, half:]], axis=1)
        return y.reshape(per * block, half).astype(jnp.bfloat16)

    def unfold(x):
        x = x.astype(jnp.float32).reshape(per, block, half)
        return jnp.concatenate(
            [x[:, :slots].reshape(per * slots, half), x[:, slots:].reshape(per * slots, half)],
            axis=1).astype(jnp.bfloat16)

    places = lax.broadcasted_iota(jnp.int32, (n, tok_rows), 0)
    named = [(places == ids[k:k + 1, :]).astype(jnp.float32) for k in range(2)]
    before = (lax.broadcasted_iota(jnp.int32, (tok_rows, tok_rows), 0)
              < lax.broadcasted_iota(jnp.int32, (tok_rows, tok_rows), 1))
    earlier = jnp.dot((named[0] + named[1]).astype(jnp.bfloat16),
                      before.astype(jnp.float32).astype(jnp.bfloat16),
                      preferred_element_type=jnp.float32)
    square = lax.broadcasted_iota(jnp.int32, (n, n), 0)
    across = lax.broadcasted_iota(jnp.int32, (n, n), 1)
    limit = jnp.sum(jnp.where(square == across, capacity[...].astype(jnp.float32), 0.0),
                    axis=1, keepdims=True)
    slot, weight = [], []
    for k in range(2):
        rank = jnp.sum(named[k] * earlier, axis=0, keepdims=True)
        most = jnp.sum(named[k] * limit, axis=0, keepdims=True)
        away = ids[k:k + 1, :] - me
        away = jnp.where(away < 0, away + n, away)
        slot.append(jnp.where(rank < most, away * slots + rank.astype(jnp.int32), -1))
        weight.append(quanta[k:k + 1, :].astype(jnp.float32) / 65536.0)

    def spread(g, values):
        at = lax.broadcasted_iota(jnp.int32, (per * slots, tok_rows), 0) + g * (per * slots)
        return (jnp.where(at == slot[0], values[0], 0.0)
                + jnp.where(at == slot[1], values[1], 0.0))

    for g in range(GROUPS):
        chosen = spread(g, (1.0, 1.0)).astype(jnp.bfloat16)
        packed[span(g), :] = fold(jnp.dot(chosen, sub_tok[...],
                                          preferred_element_type=jnp.float32))

        @pl.loop(max(1, g * per), (g + 1) * per)
        def _(i):
            outgoing(i).start()

        if g == 0:
            fetch_in.start()
            fetch_out.start()

    received[0:block, :] = packed[0:block, :]
    fetch_in.wait()
    fetch_out.wait()

    @pl.loop(0, GROUPS)
    def _(g):
        first = g * per
        low = jnp.where(g == 0, 1, first)

        @pl.loop(low, first + per)
        def _(i):
            outgoing(i).wait_recv()

        x = unfold(received[span(g), :])

        @pl.loop(0, ffe // TILE)
        def _(c):
            gate_at = pl.ds(pl.multiple_of(c * TILE, TILE), TILE)
            up_at = pl.ds(pl.multiple_of(ffe + c * TILE, TILE), TILE)
            gate = jnp.dot(x, w_in[:, gate_at], preferred_element_type=jnp.float32)
            up = jnp.dot(x, w_in[:, up_at], preferred_element_type=jnp.float32)
            hidden[:, gate_at] = (gate / (1.0 + jnp.exp(-gate)) * up).astype(jnp.bfloat16)

        act = hidden[...]
        parts = []
        for h in range(2):
            y = jnp.dot(act, w_out[:, h * half:(h + 1) * half],
                        preferred_element_type=jnp.float32)
            parts.append(y.reshape(per, slots, half))
        y = jnp.concatenate(parts, axis=1).reshape(per * block, half)
        answers[span(g), :] = y.astype(jnp.bfloat16)

        @pl.loop(low, first + per)
        def _(i):
            homeward(i).start()

    returned[0:block, :] = answers[0:block, :]
    summed = jnp.zeros((tok_rows, width), jnp.float32)
    for g in range(GROUPS):
        @pl.loop(max(1, g * per), (g + 1) * per)
        def _(i):
            homeward(i).wait_recv()

        full = spread(g, weight)
        high = full.astype(jnp.bfloat16)
        low = (full - high.astype(jnp.float32)).astype(jnp.bfloat16)
        y = unfold(returned[span(g), :])
        for part in (high, low):
            summed = summed + lax.dot_general(part, y, (((0,), (0,)), ((), ())),
                                              preferred_element_type=jnp.float32)
    head[...] = summed.astype(jnp.bfloat16)

    @pl.loop(1, n)
    def _(i):
        outgoing(i).wait_send()
        homeward(i).wait_send()


def exchange_experts(n_seq, n_sub, slots, sub_tok, ids, quanta, capacity, w_in, w_out):
    n = n_seq * n_sub
    width = w_out.shape[1]
    vmem = pl.BlockSpec(memory_space=pltpu.VMEM)
    hbm = pl.BlockSpec(memory_space=pltpu.HBM)
    rows = n * slots // GROUPS
    crossing = pltpu.VMEM((n * 2 * slots, width // 2), jnp.bfloat16)
    return pl.pallas_call(
        functools.partial(experts_kernel, n_seq, n_sub, slots),
        out_shape=jax.ShapeDtypeStruct(sub_tok.shape, jnp.bfloat16),
        in_specs=[vmem] * 4 + [hbm] * 2,
        out_specs=vmem,
        scratch_shapes=[crossing] * 4 + [
            pltpu.VMEM((rows, w_out.shape[0]), jnp.bfloat16),
            pltpu.VMEM(w_in.shape, jnp.bfloat16),
            pltpu.VMEM(w_out.shape, jnp.bfloat16),
            pltpu.SemaphoreType.DMA((2,)),
        ] + [pltpu.SemaphoreType.DMA((n,))] * 4,
        compiler_params=pltpu.CompilerParams(
            has_side_effects=True, vmem_limit_bytes=EXPERTS_VMEM),
        name="experts",
    )(sub_tok, ids, quanta, capacity, w_in, w_out)


def merge_kernel(n, head, w, out, total, sending, landed, send_sem, recv_sem):
    z = lax.axis_index("sub")
    rows, width = out.shape
    piece = rows // CHUNKS

    def target(j):
        near_low = jnp.where(j < n - 1 - z, n - 1 - j, j - (n - 1 - z))
        near_high = jnp.where(j < z, j, n - 1 - (j - z))
        return jnp.where(z < n // 2, near_low, near_high)

    barrier = pltpu.get_barrier_semaphore()

    @pl.when(z > 0)
    def _():
        pl.semaphore_signal(barrier, inc=1, device_id={"sub": z - 1}, device_id_type=MESH)

    @pl.when(z < n - 1)
    def _():
        pl.semaphore_signal(barrier, inc=1, device_id={"sub": z + 1}, device_id_type=MESH)

    pl.semaphore_wait(barrier, jnp.where(z > 0, 1, 0) + jnp.where(z < n - 1, 1, 0))

    def hop(way, t, c):
        part = pl.ds(c * piece, piece)
        return pltpu.make_async_remote_copy(
            src_ref=sending.at[t, part], dst_ref=landed.at[way, t, part],
            send_sem=send_sem.at[t, c], recv_sem=recv_sem.at[way, t, c],
            device_id={"sub": z + (1 if way == 0 else -1)}, device_id_type=MESH)

    for j in range(n):
        t = target(j)
        steps = 2 if j == 0 else 1
        for step in range(steps):
            tall = pl.ds(step * (rows // steps), rows // steps)

            @pl.loop(0, width // TILE)
            def _(k):
                cols = pl.ds(pl.multiple_of(k * TILE, TILE), TILE)
                from_cols = pl.ds(pl.multiple_of(t * width + k * TILE, TILE), TILE)
                total[t, tall, cols] = jnp.dot(head[tall, :], w[:, from_cols],
                                               preferred_element_type=jnp.float32)

            for way, source in ((0, 0), (1, n - 1)):
                @pl.when((z == source) & (t != z))
                def _():
                    for c in range(step * CHUNKS // steps, (step + 1) * CHUNKS // steps):
                        part = pl.ds(c * piece, piece)
                        sending[t, part, :] = total[t, part, :].astype(jnp.bfloat16)
                        hop(way, t, c).start()

    def relay(way, when):
        for k in range(n - 2):
            t = n - 1 - k if way == 0 else k
            inside = (z > 0) & (z < t) if way == 0 else (z < n - 1) & (z > t)

            @pl.when(inside & when)
            def _():
                for c in range(CHUNKS):
                    part = pl.ds(c * piece, piece)
                    hop(way, t, c).wait_recv()
                    sending[t, part, :] = (
                        total[t, part, :] + landed[way, t, part, :].astype(jnp.float32)
                    ).astype(jnp.bfloat16)
                    hop(way, t, c).start()

    relay(0, z < n // 2)
    relay(1, z >= 0)
    relay(0, z >= n // 2)

    for way, has in ((0, z > 0), (1, z < n - 1)):
        @pl.when(has)
        def _():
            for c in range(CHUNKS):
                part = pl.ds(c * piece, piece)
                hop(way, z, c).wait_recv()
                total[z, part, :] += landed[way, z, part, :].astype(jnp.float32)

    out[...] = total[z].astype(out.dtype)
    for t in range(n):
        @pl.when(z < t)
        def _():
            for c in range(CHUNKS):
                hop(0, t, c).wait_send()

        @pl.when(z > t)
        def _():
            for c in range(CHUNKS):
                hop(1, t, c).wait_send()


def merge_scatter(n, head, w_merge):
    rows, width = head.shape[0], w_merge.shape[1] // n
    vmem = pl.BlockSpec(memory_space=pltpu.VMEM)
    return pl.pallas_call(
        functools.partial(merge_kernel, n),
        out_shape=jax.ShapeDtypeStruct((rows, width), jnp.bfloat16),
        in_specs=[vmem, vmem],
        out_specs=vmem,
        scratch_shapes=[
            pltpu.VMEM((n, rows, width), jnp.float32),
            pltpu.VMEM((n, rows, width), jnp.bfloat16),
            pltpu.VMEM((2, n, rows, width), jnp.bfloat16),
            pltpu.SemaphoreType.DMA((n, CHUNKS)),
            pltpu.SemaphoreType.DMA((2, n, CHUNKS)),
        ],
        compiler_params=pltpu.CompilerParams(
            collective_id=1, has_side_effects=True, vmem_limit_bytes=MERGE_VMEM),
        name="merge",
    )(head, w_merge)


def body(n_seq, n_sub, tokens, w_split, w_merge, expert_in, expert_out, expert_ids, combine_q,
         capacity):
    sub_tok = jnp.dot(tokens, w_split, preferred_element_type=jnp.float32).astype(jnp.bfloat16)
    sub_tok, w_merge = lax.optimization_barrier((sub_tok, w_merge))
    tok_rows = tokens.shape[0]
    experts = capacity.shape[0]
    slot_count = -(-(3 * tok_rows // experts) // 8) * 8
    head_out = exchange_experts(
        n_seq, n_sub, slot_count, sub_tok, expert_ids[0].T, combine_q[0].T, capacity[None, :],
        expert_in[0], expert_out[0])
    return merge_scatter(n_sub, head_out, w_merge)


def solution(mesh):
    in_specs = (
        P("seq", None),
        P(None, "sub"),
        P("sub", None),
        P(("seq", "sub"), None, None),
        P(("seq", "sub"), None, None),
        P("sub", "seq", None),
        P("sub", "seq", None),
        P(),
    )
    out_specs = P("seq", "sub")
    call = functools.partial(body, mesh.shape["seq"], mesh.shape["sub"])
    return jax.shard_map(call, mesh=mesh, in_specs=in_specs, out_specs=out_specs, check_vma=False)
```
